32 devices in a mesh: dp: 4 (over y, core), mp: 8 (over z, x).
Axes of the slice: x: 2, y: 2, z: 4, core: 2. Of those that a mesh axis runs over, the one named last changes fastest.
Arguments:
- layer_input: bfloat16 [128, 256, 768], P(('dp', 'mp')), may hold values from -6 to 6
- output_cot: bfloat16 [128, 256, 768], P(('dp', 'mp')), may hold values from -6 to 6
- hidden_act: bfloat16 [128, 3072, 256], P('dp', 'mp'), may hold values from 0 to 2
- hidden_cot: bfloat16 [128, 3072, 256], P('dp', 'mp'), may hold values from -6 to 6
- lengths: int32 [128], P('dp'), may hold values from 32 to 256
- weights: float32 [768, 6144], P('dp', 'mp'), may hold values from -0.21875 to 0.21875
- moment_one: float32 [768, 6144], P('dp', 'mp'), may hold values from -3 to 3
- moment_two: float32 [768, 6144], P('dp', 'mp'), may hold values from 0.0005 to 0.02
Outputs:
- new_weights: float32 [768, 6144], P('dp', 'mp')
- new_moment_one: float32 [768, 6144], P('dp', 'mp')
- new_moment_two: float32 [768, 6144], P('dp', 'mp')
- clip_scale: float32 [128], P('dp')
The draws below stay inside these ranges and needn't reach their ends.
Inputs may be any that keep to these rules, and one draw needn't show every extreme that they name: `lengths`: slots from an example's length on are padding.
All inputs are finite; a program needn't handle non-finite values.
Results may differ from the reference program's by a relative error of at most 0.0024.
Values may be sent and summed in bfloat16 or wider, within the bound.
A program may use at most 128 MiB of HBM per device.

```python
import math
import jax
import jax.numpy as jnp
from jax import lax

D = 768
FF = 3072
SLOT = 256
STEP = 10
EXAMPLES = 128


def set_ends(values, own_key, least, top_value):
    longest = values.shape.index(max(values.shape))
    spots = []
    for shift in (0, 1):
        where = [jax.random.randint(jax.random.fold_in(own_key, axis), (), 0, length) for axis, length in enumerate(values.shape)]
        where[longest] = (where[longest] + shift) % values.shape[longest]
        spots.append(tuple(where))
    return values.at[spots[0]].set(least).at[spots[1]].set(top_value)


def steps_of(stream_key, dims, shards, least, high):
    loudness = 1.0
    for position, blocks in shards:
        heights = jax.random.uniform(jax.random.fold_in(jax.random.fold_in(stream_key, 6), position), (blocks,), jnp.float32, least / len(shards), high / len(shards))
        loudness = loudness * jnp.repeat(jnp.exp(heights), dims[position] // blocks).reshape((-1,) + (1,) * (len(dims) - 1 - position))
    return loudness


def gaussian(rng, shape, deviation, bound, split=(), kind=jnp.bfloat16):
    gain = steps_of(rng, shape, split, -0.22, 0.18) if split else 1.0
    values = jax.random.normal(rng, shape, jnp.float32) * deviation * gain
    return jnp.minimum(jnp.maximum(values, -bound), bound).astype(kind)


def setup_inputs(seed: int = 0) -> dict:
    key_of = jax.random.split(jax.random.key(seed), 9)
    return {
        "layer_input": gaussian(key_of[0], (EXAMPLES, SLOT, D), 1.0, 6.0, ((0, 32),)),
        "output_cot": gaussian(key_of[1], (EXAMPLES, SLOT, D), 1.0, 6.0, ((0, 32),)),
        "hidden_act": jnp.clip(2.0 * jax.random.uniform(key_of[2], (EXAMPLES, FF, SLOT), jnp.float32) ** steps_of(key_of[2], (EXAMPLES, FF, SLOT), ((0, 4), (1, 8)), -0.2, 0.2), 0.0, 2.0).astype(jnp.bfloat16),
        "hidden_cot": gaussian(key_of[3], (EXAMPLES, FF, SLOT), 1.0, 6.0, ((0, 4), (1, 8))),
        "lengths": set_ends(jax.random.randint(key_of[4], (EXAMPLES,), SLOT // 8, SLOT + 1), jax.random.fold_in(key_of[4], 1), SLOT // 8, SLOT).astype(jnp.int32),
        "weights": gaussian(key_of[5], (D, 2 * FF), D ** -0.5, 0.21875, ((0, 4), (1, 8)), jnp.float32),
        "moment_one": gaussian(key_of[6], (D, 2 * FF), 0.5, 3.0, ((0, 4), (1, 8)), jnp.float32),
        "moment_two": jnp.clip(jnp.exp(math.log(0.02) - 3.6888794 * jax.random.uniform(key_of[7], (D, 2 * FF), jnp.float32) ** steps_of(key_of[7], (D, 2 * FF), ((0, 4), (1, 8)), -0.2, 0.2)), 0.0005, 0.02),
    }


beta_one = 0.9
beta_two = 0.999
adam_eps = 1e-08
learn_rate = 0.001
weight_decay = 0.01

def pair_norm(example_items):
    input_rows, outcot_rows, cot_rows, hid_rows = example_items
    input_gram = jnp.dot(input_rows, input_rows.T, preferred_element_type=jnp.float32)
    cot_gram = jnp.dot(cot_rows.T, cot_rows, preferred_element_type=jnp.float32)
    outcot_gram = jnp.dot(outcot_rows, outcot_rows.T, preferred_element_type=jnp.float32)
    hid_gram = jnp.dot(hid_rows.T, hid_rows, preferred_element_type=jnp.float32)
    return jnp.sum(input_gram * cot_gram) + jnp.sum(outcot_gram * hid_gram)

def reference(layer_input, output_cot, hidden_act, hidden_cot, lengths, weights, moment_one, moment_two):
    slot_index = lax.broadcasted_iota(jnp.int32, (EXAMPLES, SLOT), 1)
    token_mask = (slot_index < lengths[:, None].astype(jnp.int32)).astype(jnp.float32)
    cot_masked = (hidden_cot.astype(jnp.float32) * token_mask[:, None, :]).astype(jnp.bfloat16)
    hid_masked = (hidden_act.astype(jnp.float32) * token_mask[:, None, :]).astype(jnp.bfloat16)
    squares = lax.map(pair_norm, (layer_input, output_cot, cot_masked, hid_masked))
    clip_limit = 0.5 * math.sqrt(2.0 * D * FF * SLOT)
    clip_scale = clip_limit / jnp.maximum(jnp.sqrt(squares), clip_limit)
    factor = clip_scale[:, None] * token_mask
    scaled_cot = (hidden_cot.astype(jnp.float32) * factor[:, None, :]).astype(jnp.bfloat16)
    scaled_hid = (hidden_act.astype(jnp.float32) * factor[:, None, :]).astype(jnp.bfloat16)
    contract = (((0, 1), (0, 2)), ((), ()))
    first_part = lax.dot_general(layer_input, scaled_cot, contract, preferred_element_type=jnp.float32)
    second_part = lax.dot_general(output_cot, scaled_hid, contract, preferred_element_type=jnp.float32)
    gradient = jnp.stack([first_part, second_part], axis=2).reshape(D, 2 * FF) / EXAMPLES
    new_moment_one = beta_one * moment_one + (1.0 - beta_one) * gradient
    new_moment_two = beta_two * moment_two + (1.0 - beta_two) * gradient * gradient
    corr_one = 1.0 - beta_one ** STEP
    corr_two = 1.0 - beta_two ** STEP
    direction = new_moment_one / corr_one / (jnp.sqrt(new_moment_two / corr_two) + adam_eps)
    new_weights = weights - learn_rate * (direction + weight_decay * weights)
    return (new_weights, new_moment_one, new_moment_two, clip_scale)
```

```python
import functools
import math

import jax
import jax.numpy as jnp
from jax import lax
from jax.experimental import pallas as pl
from jax.experimental.pallas import tpu as pltpu
from jax.sharding import PartitionSpec as P

STEP = 10

beta_one = 0.9
beta_two = 0.999
adam_eps = 1e-08
learn_rate = 0.001
weight_decay = 0.01

MESH = pl.DeviceIdType.MESH


def ring_order(count):
    fast = 1
    while fast * fast * 4 <= count and count % (fast * 2) == 0:
        fast *= 2
    slow = count // fast
    if fast == 1 or slow % 2:
        return list(range(count))
    walk = []
    for row in range(slow):
        columns = range(1, fast) if row % 2 == 0 else range(fast - 1, 0, -1)
        walk += [row * fast + column for column in columns]
    walk += [row * fast for row in range(slow - 1, -1, -1)]
    return walk


def pick(table, index):
    value = jnp.int32(table[0])
    for key in range(1, len(table)):
        value = jnp.where(index == key, jnp.int32(table[key]), value)
    return value


def kernel(
    dp,
    mp,
    clip_limit,
    input_ref,
    outcot_ref,
    cot_ref,
    hid_ref,
    mask_ref,
    grad_ref,
    clip_ref,
    input_all,
    outcot_all,
    products,
    x_buf,
    c_buf,
    sq_sum,
    sq_send,
    sq_all,
    total,
    arrived,
    ring_send,
    ring_recv,
    load_sem,
    sq_send_sem,
    sq_recv_sem,
    rs_send_sem,
    rs_recv_sem,
):
    own = input_ref.shape[0]
    examples, units = cot_ref.shape[0], cot_ref.shape[1]
    width = input_ref.shape[2]
    rows = grad_ref.shape[1]
    my_dp, my_mp = lax.axis_index("dp"), lax.axis_index("mp")
    order = ring_order(mp)
    place = [order.index(m) for m in range(mp)]
    pos = pick(place, my_mp)
    following = pick(order, lax.rem(pos + 1, mp))
    previous = pick(order, lax.rem(pos + mp - 1, mp))
    targets = (following, previous)
    own_refs = (input_ref, outcot_ref)
    all_refs = (input_all, outcot_all)
    hidden_refs = (cot_ref, hid_ref)

    barrier = pltpu.get_barrier_semaphore()
    for k in range(1, mp):
        peer = lax.rem(my_mp + k, mp)
        pl.semaphore_signal(barrier, inc=1, device_id=(my_dp, peer), device_id_type=MESH)
    for k in range(1, dp):
        peer = lax.rem(my_dp + k, dp)
        pl.semaphore_signal(barrier, inc=1, device_id=(peer, my_mp), device_id_type=MESH)
    pl.semaphore_wait(barrier, mp + dp - 2)

    def origins(step):
        return (
            pick(order, lax.rem(pos - step + mp, mp)),
            pick(order, lax.rem(pos + step, mp)),
        )

    def hop(k, source, example, step, chunk):
        return pltpu.make_async_remote_copy(
            src_ref=source,
            dst_ref=all_refs[k].at[example],
            send_sem=ring_send.at[k, step, chunk],
            recv_sem=ring_recv.at[k, step, chunk],
            device_id=(my_dp, targets[k]),
            device_id_type=MESH,
        )

    def load_hidden(k, example):
        return pltpu.make_async_copy(hidden_refs[k].at[example], c_buf.at[k], load_sem.at[k, 0])

    def load_rows(k, source):
        return pltpu.make_async_copy(source, x_buf.at[k], load_sem.at[k, 1])

    def product(k, example):
        mask = mask_ref[pl.ds(example, 1), :]
        masked = (c_buf[k].astype(jnp.float32) * mask).astype(jnp.bfloat16)
        piece = jnp.dot(masked, x_buf[k], preferred_element_type=jnp.float32)
        products[k, example] = piece.astype(jnp.bfloat16)
        sq_sum[pl.ds(example, 1), :] += jnp.sum(piece * piece, axis=0, keepdims=True)

    for chunk in range(own):
        for k in range(2):
            hop(k, own_refs[k].at[chunk], my_mp * own + chunk, 1, chunk).start()

    sq_sum[...] = jnp.zeros_like(sq_sum)

    def own_step(chunk, carry):
        example = my_mp * own + chunk
        for k in range(2):
            load_hidden(k, example).start()
            load_rows(k, own_refs[k].at[chunk]).start()
        for k in range(2):
            load_hidden(k, example).wait()
            load_rows(k, own_refs[k].at[chunk]).wait()
            product(k, example)
        return carry

    lax.fori_loop(0, own, own_step, 0)

    def ring_step(index, carry):
        step, chunk = lax.div(index, own), lax.rem(index, own)
        spots = [origin * own + chunk for origin in origins(step)]
        for k in range(2):
            load_hidden(k, spots[k]).start()
        for k in range(2):
            here = all_refs[k].at[spots[k]]
            hop(k, here, spots[k], step, chunk).wait_recv()

            @pl.when(step < mp - 1)
            def _():
                hop(k, here, spots[k], step + 1, chunk).start()

            load_rows(k, here).start()
        for k in range(2):
            load_hidden(k, spots[k]).wait()
            load_rows(k, all_refs[k].at[spots[k]]).wait()
            product(k, spots[k])
        return carry

    lax.fori_loop(own, mp * own, ring_step, 0)

    sums = jnp.broadcast_to(jnp.sum(sq_sum[...], axis=1, keepdims=True), sq_send.shape)
    sq_send[...] = sums
    sq_all[my_mp] = sums

    def share(k):
        return pltpu.make_async_remote_copy(
            src_ref=sq_send,
            dst_ref=sq_all.at[my_mp],
            send_sem=sq_send_sem.at[k],
            recv_sem=sq_recv_sem.at[k],
            device_id=(my_dp, lax.rem(my_mp + k, mp)),
            device_id_type=MESH,
        )

    for k in range(1, mp):
        share(k).start()

    def drain(index, carry):
        step, chunk = lax.div(index, own), lax.rem(index, own)
        for k in range(2):
            hop(k, own_refs[k].at[0], 0, step, chunk).wait_send()
        return carry

    lax.fori_loop(own, mp * own, drain, 0)
    for k in range(1, mp):
        share(k).wait()

    squares = sq_all[0]
    for source in range(1, mp):
        squares = squares + sq_all[source]
    clip_ref[...] = clip_limit / jnp.maximum(jnp.sqrt(squares), clip_limit)

    tile = 128
    unit_tile = tile if units % tile == 0 else units
    unit_tiles = units // unit_tile

    def scatter(k, ahead):
        peer = lax.rem(my_dp + ahead, dp)
        return pltpu.make_async_remote_copy(
            src_ref=total.at[k, pl.ds(pl.multiple_of(peer * rows, 16), rows), :],
            dst_ref=arrived.at[ahead, k],
            send_sem=rs_send_sem.at[k, ahead],
            recv_sem=rs_recv_sem.at[k, ahead],
            device_id=(peer, my_mp),
            device_id_type=MESH,
        )

    for k in range(2):

        def weigh(index, carry):
            column = pl.ds(pl.multiple_of(lax.div(index, unit_tiles) * tile, tile), tile)
            if unit_tiles == 1:
                unit = pl.ds(0, unit_tile)
            else:
                unit = pl.ds(pl.multiple_of(lax.rem(index, unit_tiles) * tile, tile), tile)
            value = jnp.zeros((unit_tile, tile), jnp.float32)
            for example in range(examples):
                value += clip_ref[example : example + 1, :] * products[
                    k, example, unit, column
                ].astype(jnp.float32)
            total[k, column, unit] = value.T.astype(jnp.bfloat16)
            return carry

        lax.fori_loop(0, width // tile * unit_tiles, weigh, 0)
        for ahead in range(1, dp):
            scatter(k, ahead).start()

    for k in range(2):
        grad = total[k, pl.ds(pl.multiple_of(my_dp * rows, 16), rows), :].astype(jnp.float32)
        for ahead in range(1, dp):
            scatter(k, ahead).wait()
            grad += arrived[ahead, k].astype(jnp.float32)
        grad_ref[k] = grad


def clipped_sum(dp, mp, layer_input, output_cot, hidden_cot, hidden_act, mask):
    own, slots, width = layer_input.shape
    examples, units, _ = hidden_cot.shape
    clip_limit = 0.5 * math.sqrt(2.0 * width * units * mp * slots)
    rows = width // dp
    anywhere = pl.BlockSpec(memory_space=pl.ANY)
    vmem = pl.BlockSpec(memory_space=pltpu.VMEM)
    dma = pltpu.SemaphoreType.DMA
    grad, clip, _, _ = pl.pallas_call(
        functools.partial(kernel, dp, mp, clip_limit),
        out_shape=(
            jax.ShapeDtypeStruct((2, rows, units), jnp.float32),
            jax.ShapeDtypeStruct((examples, 128), jnp.float32),
            jax.ShapeDtypeStruct((own * mp, slots, width), jnp.bfloat16),
            jax.ShapeDtypeStruct((own * mp, slots, width), jnp.bfloat16),
        ),
        in_specs=[anywhere] * 4 + [vmem],
        out_specs=(vmem, vmem, anywhere, anywhere),
        scratch_shapes=[
            pltpu.VMEM((2, examples, units, width), jnp.bfloat16),
            pltpu.VMEM((2, slots, width), jnp.bfloat16),
            pltpu.VMEM((2, units, slots), jnp.bfloat16),
            pltpu.VMEM((examples, width), jnp.float32),
            pltpu.VMEM((examples, 128), jnp.float32),
            pltpu.VMEM((mp, examples, 128), jnp.float32),
            pltpu.VMEM((2, width, units), jnp.bfloat16),
            pltpu.VMEM((dp, 2, rows, units), jnp.bfloat16),
            dma((2, mp, own)),
            dma((2, mp, own)),
            dma((2, 2)),
            dma((mp,)),
            dma((mp,)),
            dma((2, dp)),
            dma((2, dp)),
        ],
        compiler_params=pltpu.CompilerParams(
            collective_id=0, has_side_effects=True, vmem_limit_bytes=60 * 1024 * 1024
        ),
    )(layer_input, output_cot, hidden_cot, hidden_act, mask)
    return grad, clip


def local(
    dp, mp, layer_input, output_cot, hidden_act, hidden_cot, lengths, weights, moment_one, moment_two
):
    slots = layer_input.shape[1]
    slot_index = lax.broadcasted_iota(jnp.int32, (lengths.shape[0], slots), 1)
    mask = (slot_index < lengths[:, None]).astype(jnp.float32)
    summed, clip = clipped_sum(dp, mp, layer_input, output_cot, hidden_cot, hidden_act, mask)
    clip_scale = clip[:, 0]
    gradient = jnp.stack([summed[0], summed[1]], axis=2).reshape(weights.shape)
    gradient = gradient / (lengths.shape[0] * dp)
    new_moment_one = beta_one * moment_one + (1.0 - beta_one) * gradient
    new_moment_two = beta_two * moment_two + (1.0 - beta_two) * gradient * gradient
    corr_one = 1.0 - beta_one**STEP
    corr_two = 1.0 - beta_two**STEP
    direction = new_moment_one / corr_one / (jnp.sqrt(new_moment_two / corr_two) + adam_eps)
    new_weights = weights - learn_rate * (direction + weight_decay * weights)
    return (new_weights, new_moment_one, new_moment_two, clip_scale)


def solution(mesh):
    return jax.shard_map(
        functools.partial(local, mesh.shape["dp"], mesh.shape["mp"]),
        mesh=mesh,
        in_specs=(
            P(("dp", "mp"), None, None),
            P(("dp", "mp"), None, None),
            P("dp", "mp", None),
            P("dp", "mp", None),
            P("dp"),
            P("dp", "mp"),
            P("dp", "mp"),
            P("dp", "mp"),
        ),
        out_specs=(P("dp", "mp"), P("dp", "mp"), P("dp", "mp"), P("dp")),
        check_vma=False,
    )
```
